32 devices in a mesh: groups: 2 (over y), band: 4 (over z), chan: 4 (over x, core).
Axes of the slice: x: 2, y: 2, z: 4, core: 2. Of those that a mesh axis runs over, the one named last changes fastest.
Arguments:
- slide_region: float32 [16, 32, 8192], P('chan', ('groups', 'band')), parts along dimension 1, may hold values from -6 to 6
- row_taps: float32 [16, 257], P('chan'), may hold values from -0.375 to 0.375
- column_taps: float32 [16, 257], replicated, may hold values from -0.375 to 0.375
- channel_mix: float32 [16, 16], replicated, may hold values from -1.5 to 1.5
Outputs:
- filtered: float32 [16, 32, 8192], P('chan', ('groups', 'band')), parts along dimension 1
The draws below stay inside these ranges and needn't reach their ends.
There are 2 independent parts, one for each index of `groups`. The reference program is written for one: setup_inputs(seed, part) draws one part's arguments, and reference() takes and returns one part's arrays. A program takes and returns all parts, laid end to end along the dimension named above; an argument that names none is the same for every part. Nothing has to cross between parts.
All inputs are finite; a program needn't handle non-finite values.
Results may differ from the reference program's by a relative error of at most 0.00007.
Values sent between devices are 32-bit elements; how exact they have to be, the bound alone decides.
A program may use at most 64 MiB of HBM per device.

```python
import jax
import jax.numpy as jnp
from jax import lax

C = 16
TAPS = 257
COLS = 8192
ROWS = 16


def block_scale(own_key, shape, split, least, largest):
    loudness, own = 1.0, jax.random.fold_in(own_key, 6)
    for axis_at, shards_of in split:
        draws = jnp.exp(jax.random.uniform(jax.random.fold_in(own, axis_at), (shards_of,), jnp.float32, least / len(split), largest / len(split)))
        loudness = loudness * jnp.repeat(draws, shape[axis_at] // shards_of).reshape([-1 if axis == axis_at else 1 for axis in range(len(shape))])
    return loudness


def scatter_about(own_key, shape, spread, reach, shards=(), dtype=jnp.bfloat16):
    loudness = block_scale(own_key, shape, shards, -0.22, 0.18) if shards else 1.0
    drawn = jax.random.normal(own_key, shape, jnp.float32) * spread * loudness
    return jnp.minimum(jnp.maximum(drawn, -reach), reach).astype(dtype)


def setup_inputs(seed: int = 0, part: int = 0) -> dict:
    arg_keys = jax.random.split(jax.random.key(seed), 5)
    part_splits = jax.random.split(jax.random.fold_in(arg_keys[4], part), 5)
    slide_region = scatter_about(part_splits[0], (C, ROWS, COLS), 1.0, 6.0, ((0, 4), (1, 4)), jnp.float32)
    row_taps = scatter_about(arg_keys[1], (C, TAPS), TAPS ** -0.5, 0.375, ((0, 4),), jnp.float32)
    column_taps = scatter_about(arg_keys[2], (C, TAPS), TAPS ** -0.5, 0.375, (), jnp.float32)
    channel_mix = scatter_about(arg_keys[3], (C, C), C ** -0.5, 1.5, (), jnp.float32)
    return dict(slide_region=slide_region, row_taps=row_taps, column_taps=column_taps, channel_mix=channel_mix)


def depthwise(signal, filter_taps, horizontal):
    channels = signal.shape[0]
    margin = (filter_taps.shape[1] - 1) // 2
    if horizontal:
        kernel = filter_taps[:, None, None, :]
        padding = ((0, 0), (margin, margin))
    else:
        kernel = filter_taps[:, None, :, None]
        padding = ((margin, margin), (0, 0))
    result = lax.conv_general_dilated(signal[None], kernel, (1, 1), padding,
                                      dimension_numbers=("NCHW", "OIHW", "NCHW"),
                                      feature_group_count=channels,
                                      precision=lax.Precision.HIGHEST)
    return result[0]


def reference(slide_region, row_taps, column_taps, channel_mix):
    across = depthwise(slide_region, row_taps, True)
    vertical = depthwise(across, column_taps, False)
    return jnp.einsum("oc,chw->ohw", channel_mix, vertical, precision=lax.Precision.HIGHEST)
```

```python
import functools

import jax
import jax.numpy as jnp
from jax import lax
from jax.experimental import pallas as pl
from jax.experimental.pallas import tpu as pltpu
from jax.sharding import PartitionSpec as P

precise = lax.Precision.HIGHEST


def band_tables(filter_taps, tile_size):
    channels, length = filter_taps.shape
    margin = (length - 1) // 2
    period = 4 * tile_size
    border = 3 * tile_size + length
    widened = jnp.pad(filter_taps, ((0, 0), (border, border)))
    lowest = margin - tile_size + border
    window = widened[:, lowest : lowest + 3 * tile_size]
    vector = jnp.pad(window, ((0, 0), (0, tile_size)))
    repeated = jnp.tile(vector, (1, tile_size))[:, : tile_size * (period - 1)]
    toeplitz = repeated.reshape(channels, tile_size, period - 1)[:, :, : 3 * tile_size]
    stacked = jnp.transpose(toeplitz, (0, 2, 1))
    return stacked.reshape(channels, 3, tile_size, tile_size)


def along_columns(signal, filter_taps):
    tile_size = 128
    tables = band_tables(filter_taps, tile_size)
    channels, row_count, col_count = signal.shape
    tile_count = col_count // tile_size
    tiled = signal.reshape(channels, row_count, tile_count, tile_size)
    padded = jnp.pad(tiled, ((0, 0), (0, 0), (1, 1), (0, 0)))
    result = jnp.einsum(
        "crti,cij->crtj", padded[:, :, 0:tile_count], tables[:, 0], precision=precise
    )
    result = result + jnp.einsum(
        "crti,cij->crtj", padded[:, :, 1 : tile_count + 1], tables[:, 1], precision=precise
    )
    result = result + jnp.einsum(
        "crti,cij->crtj", padded[:, :, 2:], tables[:, 2], precision=precise
    )
    return result.reshape(channels, row_count, col_count)


def along_rows(signal, filter_taps):
    channels, row_count, col_count = signal.shape
    tile_size = 128 if row_count % 128 == 0 else row_count
    tables = band_tables(filter_taps, tile_size)
    tile_count = row_count // tile_size
    tiled = signal.reshape(channels, tile_count, tile_size, col_count)
    padded = jnp.pad(tiled, ((0, 0), (1, 1), (0, 0), (0, 0)))
    result = jnp.einsum("ctiw,cij->ctjw", padded[:, 0:tile_count], tables[:, 0], precision=precise)
    result = result + jnp.einsum(
        "ctiw,cij->ctjw", padded[:, 1 : tile_count + 1], tables[:, 1], precision=precise
    )
    result = result + jnp.einsum("ctiw,cij->ctjw", padded[:, 2:], tables[:, 2], precision=precise)
    return result.reshape(channels, row_count, col_count)


def on_device(slide_region, row_taps, column_taps, channel_mix):
    local_channels = slide_region.shape[0]
    across = along_columns(slide_region, row_taps)
    column_band = lax.all_to_all(across, "band", split_axis=2, concat_axis=1, tiled=True)
    first_channel = lax.axis_index("chan") * local_channels
    own_taps = lax.dynamic_slice_in_dim(column_taps, first_channel, local_channels, 0)
    vertical = along_rows(column_band, own_taps)
    own_mixing = lax.dynamic_slice_in_dim(channel_mix, first_channel, local_channels, 0)
    blended = jnp.einsum(
        "oc,chw->ohw",
        own_mixing,
        lax.all_gather(vertical, "chan", axis=0, tiled=True),
        precision=precise,
    )
    return lax.all_to_all(blended, "band", split_axis=1, concat_axis=2, tiled=True)


LANES = 128
CHUNKS = 2


def split(value):
    high = value.astype(jnp.bfloat16)
    return high, (value - high.astype(jnp.float32)).astype(jnp.bfloat16)


def product(left, right, dims):
    (left_high, left_low), (right_high, right_low) = left, right
    dot = functools.partial(
        lax.dot_general, dimension_numbers=(dims, ((), ())), preferred_element_type=jnp.float32
    )
    return dot(left_high, right_high) + (dot(left_low, right_high) + dot(left_high, right_low))


def filter_table(taps):
    shape = (LANES, LANES)
    lane = lax.broadcasted_iota(jnp.int32, shape, 1)
    row = lax.broadcasted_iota(jnp.int32, shape, 0)
    first, second = (
        pltpu.roll(
            jnp.broadcast_to(taps[:, at : at + LANES], shape), 0, 1, stride=1, stride_axis=0
        )
        for at in (0, LANES)
    )
    last = jnp.broadcast_to(taps[:, 2 * LANES :], shape)
    zero = jnp.zeros(shape, jnp.float32)
    return jnp.concatenate(
        [
            jnp.where(lane >= row, first, zero),
            jnp.where(lane >= row, second, first),
            jnp.where(lane == row, last, jnp.where(lane < row, second, zero)),
        ],
        axis=1,
    )


def mixing_table(column_taps, channel_mix, chans, bands, local_channels, local_rows):
    channels = chans * local_channels
    height = bands * local_rows
    block = local_channels * local_rows
    size = chans * bands * block
    margin = (column_taps.shape[1] - 1) // 2

    def coordinates(index):
        device, inner = index // block, index % block
        return (
            local_channels * (device % chans) + inner // local_rows,
            local_rows * (device // chans) + inner % local_rows,
        )

    tall = (size, channels)
    wide = (channels, size)
    pick_tall = (
        coordinates(lax.broadcasted_iota(jnp.int32, tall, 0))[0]
        == lax.broadcasted_iota(jnp.int32, tall, 1)
    ).astype(jnp.float32)
    pick_wide = (
        coordinates(lax.broadcasted_iota(jnp.int32, wide, 1))[0]
        == lax.broadcasted_iota(jnp.int32, wide, 0)
    ).astype(jnp.float32)
    weights = jnp.dot(
        jnp.dot(pick_tall, channel_mix, precision=precise), pick_wide, precision=precise
    )
    taps = lax.dot_general(
        column_taps[:, : 2 * margin],
        pick_wide,
        (((0,), (0,)), ((), ())),
        precision=precise,
    )
    square = (size, size)
    apart = (
        coordinates(lax.broadcasted_iota(jnp.int32, square, 1))[1]
        - coordinates(lax.broadcasted_iota(jnp.int32, square, 0))[1]
    )
    spread = jnp.zeros(square, jnp.float32)
    for distance in range(1 - height, height):
        at = margin + distance
        spread = jnp.where(apart == distance, taps[at : at + 1, :], spread)
    return weights * spread


def fused_kernel(
    chans, bands, x_hbm, row_taps, column_taps, channel_mix, out_hbm,
    x_buf, send_one, recv_one, send_two, mixing,
    in_sem, own_sem, send_one_sem, recv_one_sem, send_two_sem, recv_two_sem,
):
    local_channels, x_rows, _ = x_hbm.shape
    devices, _, block_rows, _ = send_two.shape
    tiles = send_one.shape[1]
    local_rows = block_rows // tiles
    chan, band = lax.axis_index("chan"), lax.axis_index("band")
    me = band * chans + chan

    barrier = pltpu.get_barrier_semaphore()
    peers = []
    for band_step in sorted(range(bands), key=lambda step: (-(2 * step // bands), step)):
        for chan_step in range(chans):
            if band_step or chan_step:
                peers.append((chan ^ chan_step, band ^ band_step))
    names = [{"chan": to_chan, "band": to_band} for to_chan, to_band in peers]
    slots = [to_band * chans + to_chan for to_chan, to_band in peers]
    for name in names:
        pl.semaphore_signal(barrier, inc=1, device_id=name, device_id_type=pl.DeviceIdType.MESH)

    loads = [
        pltpu.make_async_copy(x_hbm.at[c], x_buf.at[c, pl.ds(8, x_rows)], in_sem.at[c])
        for c in range(local_channels)
    ]
    for load in loads:
        load.start()
    edge = jnp.zeros((8, LANES), jnp.float32)
    for c in range(local_channels):
        x_buf[c, 0:8, :] = edge
        x_buf[c, x_rows + 8 : x_rows + 16, :] = edge

    for c in range(local_channels):
        table = split(filter_table(row_taps[c : c + 1, :]))
        loads[c].wait()
        window = jnp.concatenate(
            [
                x_buf[c, 8 + (k - 1) * local_rows : 8 + (k - 1) * local_rows + x_rows, :]
                for k in range(3)
            ],
            axis=1,
        )
        filtered = product(split(window), table, ((1,), (1,)))
        for device in range(devices):
            for tile in range(tiles):
                at = (device * tiles + tile) * local_rows
                send_one[device, tile, c * local_rows : (c + 1) * local_rows, :] = filtered[
                    at : at + local_rows, :
                ]

    pl.semaphore_wait(barrier, len(peers))
    step = tiles // CHUNKS
    copies = []
    for chunk in range(CHUNKS):
        part = pl.ds(chunk * step, step)
        for name, slot in zip(names, slots):
            copy = pltpu.make_async_remote_copy(
                src_ref=send_one.at[slot, part],
                dst_ref=recv_one.at[part, me],
                send_sem=send_one_sem.at[chunk, slot],
                recv_sem=recv_one_sem.at[chunk, me],
                device_id=name,
                device_id_type=pl.DeviceIdType.MESH,
            )
            copy.start()
            copies.append(copy)
    recv_one[:, me] = send_one[me]

    table = mixing_table(
        column_taps[...], channel_mix[...], chans, bands, local_channels, local_rows
    )
    mixing[0], mixing[1] = split(table)

    rows = step * local_rows
    own = []
    for chunk in range(CHUNKS):
        part = pl.ds(chunk * step, step)
        for slot in slots:
            landed = recv_one.at[part, slot]
            pltpu.make_async_copy(landed, landed, recv_one_sem.at[chunk, slot]).wait()
        columns = jnp.concatenate(
            [
                recv_one[chunk * step + tile].reshape(mixing.shape[1], LANES)
                for tile in range(step)
            ],
            axis=1,
        )
        mixed = product((mixing[0], mixing[1]), split(columns), ((1,), (0,)))
        for device in range(devices):
            for c in range(local_channels):
                at = (device * local_channels + c) * local_rows
                for tile in range(step):
                    to = (chunk * step + tile) * local_rows
                    send_two[device, c, to : to + local_rows, :] = mixed[
                        at : at + local_rows, tile * LANES : (tile + 1) * LANES
                    ]
        here = pl.ds(chunk * rows, rows)
        there = pl.ds(pl.multiple_of(me * block_rows + chunk * rows, 8), rows)
        for name, slot in zip(names, slots):
            copy = pltpu.make_async_remote_copy(
                src_ref=send_two.at[slot, :, here],
                dst_ref=out_hbm.at[:, there],
                send_sem=send_two_sem.at[chunk, slot],
                recv_sem=recv_two_sem.at[chunk, me],
                device_id=name,
                device_id_type=pl.DeviceIdType.MESH,
            )
            copy.start()
            copies.append(copy)
        copy = pltpu.make_async_copy(
            send_two.at[me, :, here], out_hbm.at[:, there], own_sem.at[chunk]
        )
        copy.start()
        own.append(copy)

    for chunk in range(CHUNKS):
        for slot in slots:
            landed = out_hbm.at[
                :, pl.ds(pl.multiple_of(slot * block_rows + chunk * rows, 8), rows)
            ]
            pltpu.make_async_copy(landed, landed, recv_two_sem.at[chunk, slot]).wait()
        own[chunk].wait()
    for copy in copies:
        copy.wait_send()


def fused(chans, bands, slide_region, row_taps, column_taps, channel_mix):
    local_channels, local_rows, width = slide_region.shape
    devices = chans * bands
    total_tiles = width // LANES
    tiles = total_tiles // devices
    block = local_channels * local_rows
    tiled = slide_region.reshape(local_channels, local_rows, total_tiles, LANES)
    tiled = tiled.transpose(0, 2, 1, 3).reshape(local_channels, total_tiles * local_rows, LANES)
    vmem = pl.BlockSpec(memory_space=pltpu.VMEM)
    anywhere = pl.BlockSpec(memory_space=pl.ANY)
    dma = pltpu.SemaphoreType.DMA
    out = pl.pallas_call(
        functools.partial(fused_kernel, chans, bands),
        out_shape=jax.ShapeDtypeStruct(tiled.shape, jnp.float32),
        in_specs=[anywhere, vmem, vmem, vmem],
        out_specs=anywhere,
        scratch_shapes=[
            pltpu.VMEM((local_channels, tiled.shape[1] + 16, LANES), jnp.float32),
            pltpu.VMEM((devices, tiles, block, LANES), jnp.float32),
            pltpu.VMEM((tiles, devices, block, LANES), jnp.float32),
            pltpu.VMEM((devices, local_channels, tiles * local_rows, LANES), jnp.float32),
            pltpu.VMEM((2, devices * block, devices * block), jnp.bfloat16),
            dma((local_channels,)),
            dma((CHUNKS,)),
            dma((CHUNKS, devices)),
            dma((CHUNKS, devices)),
            dma((CHUNKS, devices)),
            dma((CHUNKS, devices)),
        ],
        compiler_params=pltpu.CompilerParams(collective_id=0, has_side_effects=True),
    )(tiled, row_taps, column_taps, channel_mix)
    out = out.reshape(local_channels, total_tiles, local_rows, LANES)
    return out.transpose(0, 2, 1, 3).reshape(slide_region.shape)


def power_of_two(number):
    return number & (number - 1) == 0


def program(chans, bands, slide_region, row_taps, column_taps, channel_mix):
    local_channels, local_rows, width = slide_region.shape
    devices = chans * bands
    margin = (row_taps.shape[1] - 1) // 2
    fits = (
        power_of_two(chans)
        and power_of_two(bands)
        and width % (devices * LANES * CHUNKS) == 0
        and margin == LANES
        and column_taps.shape[1] == row_taps.shape[1]
        and local_rows == 4
        and local_rows * bands <= margin
        and local_channels * local_rows % 8 == 0
        and width // (devices * LANES * CHUNKS) * local_rows % 8 == 0
        and devices * local_channels * local_rows <= 512
    )
    if fits:
        return fused(chans, bands, slide_region, row_taps, column_taps, channel_mix)
    return on_device(slide_region, row_taps, column_taps, channel_mix)


def solution(mesh):
    in_specs = (P("chan", ("groups", "band"), None), P("chan", None), P(), P())
    out_specs = P("chan", ("groups", "band"), None)
    return jax.shard_map(
        functools.partial(program, mesh.shape["chan"], mesh.shape["band"]),
        mesh=mesh,
        in_specs=in_specs,
        out_specs=out_specs,
        check_vma=False,
    )
```

```python
import functools

import jax
import jax.numpy as jnp
from jax import lax
from jax.experimental import pallas as pl
from jax.experimental.pallas import tpu as pltpu
from jax.sharding import PartitionSpec as P

precise = lax.Precision.HIGHEST


def band_tables(filter_taps, tile_size):
    channels, length = filter_taps.shape
    margin = (length - 1) // 2
    period = 4 * tile_size
    border = 3 * tile_size + length
    widened = jnp.pad(filter_taps, ((0, 0), (border, border)))
    lowest = margin - tile_size + border
    window = widened[:, lowest : lowest + 3 * tile_size]
    vector = jnp.pad(window, ((0, 0), (0, tile_size)))
    repeated = jnp.tile(vector, (1, tile_size))[:, : tile_size * (period - 1)]
    toeplitz = repeated.reshape(channels, tile_size, period - 1)[:, :, : 3 * tile_size]
    stacked = jnp.transpose(toeplitz, (0, 2, 1))
    return stacked.reshape(channels, 3, tile_size, tile_size)


def along_columns(signal, filter_taps):
    tile_size = 128
    tables = band_tables(filter_taps, tile_size)
    channels, row_count, col_count = signal.shape
    tile_count = col_count // tile_size
    tiled = signal.reshape(channels, row_count, tile_count, tile_size)
    padded = jnp.pad(tiled, ((0, 0), (0, 0), (1, 1), (0, 0)))
    result = jnp.einsum(
        "crti,cij->crtj", padded[:, :, 0:tile_count], tables[:, 0], precision=precise
    )
    result = result + jnp.einsum(
        "crti,cij->crtj", padded[:, :, 1 : tile_count + 1], tables[:, 1], precision=precise
    )
    result = result + jnp.einsum(
        "crti,cij->crtj", padded[:, :, 2:], tables[:, 2], precision=precise
    )
    return result.reshape(channels, row_count, col_count)


def along_rows(signal, filter_taps):
    channels, row_count, col_count = signal.shape
    tile_size = 128 if row_count % 128 == 0 else row_count
    tables = band_tables(filter_taps, tile_size)
    tile_count = row_count // tile_size
    tiled = signal.reshape(channels, tile_count, tile_size, col_count)
    padded = jnp.pad(tiled, ((0, 0), (1, 1), (0, 0), (0, 0)))
    result = jnp.einsum("ctiw,cij->ctjw", padded[:, 0:tile_count], tables[:, 0], precision=precise)
    result = result + jnp.einsum(
        "ctiw,cij->ctjw", padded[:, 1 : tile_count + 1], tables[:, 1], precision=precise
    )
    result = result + jnp.einsum("ctiw,cij->ctjw", padded[:, 2:], tables[:, 2], precision=precise)
    return result.reshape(channels, row_count, col_count)


def on_device(slide_region, row_taps, column_taps, channel_mix):
    local_channels = slide_region.shape[0]
    across = along_columns(slide_region, row_taps)
    column_band = lax.all_to_all(across, "band", split_axis=2, concat_axis=1, tiled=True)
    first_channel = lax.axis_index("chan") * local_channels
    own_taps = lax.dynamic_slice_in_dim(column_taps, first_channel, local_channels, 0)
    vertical = along_rows(column_band, own_taps)
    own_mixing = lax.dynamic_slice_in_dim(channel_mix, first_channel, local_channels, 0)
    blended = jnp.einsum(
        "oc,chw->ohw",
        own_mixing,
        lax.all_gather(vertical, "chan", axis=0, tiled=True),
        precision=precise,
    )
    return lax.all_to_all(blended, "band", split_axis=1, concat_axis=2, tiled=True)


LANES = 128
CHUNKS = 2


def split(value):
    high = value.astype(jnp.bfloat16)
    return high, (value - high.astype(jnp.float32)).astype(jnp.bfloat16)


def product(left, right, dims):
    (left_high, left_low), (right_high, right_low) = left, right
    dot = functools.partial(
        lax.dot_general, dimension_numbers=(dims, ((), ())), preferred_element_type=jnp.float32
    )
    return dot(left_high, right_high) + (dot(left_low, right_high) + dot(left_high, right_low))


def filter_table(taps):
    shape = (LANES, LANES)
    lane = lax.broadcasted_iota(jnp.int32, shape, 1)
    row = lax.broadcasted_iota(jnp.int32, shape, 0)
    first, second = (
        pltpu.roll(
            jnp.broadcast_to(taps[:, at : at + LANES], shape), 0, 1, stride=1, stride_axis=0
        )
        for at in (0, LANES)
    )
    last = jnp.broadcast_to(taps[:, 2 * LANES :], shape)
    zero = jnp.zeros(shape, jnp.float32)
    return jnp.concatenate(
        [
            jnp.where(lane >= row, first, zero),
            jnp.where(lane >= row, second, first),
            jnp.where(lane == row, last, jnp.where(lane < row, second, zero)),
        ],
        axis=1,
    )


def mixing_table(column_taps, channel_mix, chans, bands, local_channels, local_rows):
    channels = chans * local_channels
    height = bands * local_rows
    block = local_channels * local_rows
    size = chans * bands * block
    margin = (column_taps.shape[1] - 1) // 2

    def coordinates(index):
        device, inner = index // block, index % block
        return (
            local_channels * (device % chans) + inner // local_rows,
            local_rows * (device // chans) + inner % local_rows,
        )

    tall = (size, channels)
    wide = (channels, size)
    pick_tall = (
        coordinates(lax.broadcasted_iota(jnp.int32, tall, 0))[0]
        == lax.broadcasted_iota(jnp.int32, tall, 1)
    ).astype(jnp.float32)
    pick_wide = (
        coordinates(lax.broadcasted_iota(jnp.int32, wide, 1))[0]
        == lax.broadcasted_iota(jnp.int32, wide, 0)
    ).astype(jnp.float32)
    weights = jnp.dot(
        jnp.dot(pick_tall, channel_mix, precision=precise), pick_wide, precision=precise
    )
    taps = lax.dot_general(
        column_taps[:, : 2 * margin],
        pick_wide,
        (((0,), (0,)), ((), ())),
        precision=precise,
    )
    square = (size, size)
    apart = (
        coordinates(lax.broadcasted_iota(jnp.int32, square, 1))[1]
        - coordinates(lax.broadcasted_iota(jnp.int32, square, 0))[1]
    )
    spread = jnp.zeros(square, jnp.float32)
    for distance in range(1 - height, height):
        at = margin + distance
        spread = jnp.where(apart == distance, taps[at : at + 1, :], spread)
    return weights * spread


def fused_kernel(
    chans, bands, x_hbm, row_taps, column_taps, channel_mix, out_ref,
    x_buf, send_one, recv_one, send_two, mixing,
    in_sem, send_one_sem, recv_one_sem, send_two_sem, recv_two_sem,
):
    local_channels, x_rows, _ = x_hbm.shape
    devices, _, block_rows, _ = send_two.shape
    tiles = send_one.shape[1]
    local_rows = block_rows // tiles
    chan, band = lax.axis_index("chan"), lax.axis_index("band")
    me = band * chans + chan

    barrier = pltpu.get_barrier_semaphore()
    peers = []
    for band_step in sorted(range(bands), key=lambda step: (-(2 * step // bands), step)):
        for chan_step in range(chans):
            if band_step or chan_step:
                peers.append((chan ^ chan_step, band ^ band_step))
    names = [{"chan": to_chan, "band": to_band} for to_chan, to_band in peers]
    slots = [to_band * chans + to_chan for to_chan, to_band in peers]
    for name in names:
        pl.semaphore_signal(barrier, inc=1, device_id=name, device_id_type=pl.DeviceIdType.MESH)

    loads = [
        pltpu.make_async_copy(x_hbm.at[c], x_buf.at[c, pl.ds(8, x_rows)], in_sem.at[c])
        for c in range(local_channels)
    ]
    for load in loads:
        load.start()
    edge = jnp.zeros((8, LANES), jnp.float32)
    for c in range(local_channels):
        x_buf[c, 0:8, :] = edge
        x_buf[c, x_rows + 8 : x_rows + 16, :] = edge

    for c in range(local_channels):
        table = split(filter_table(row_taps[c : c + 1, :]))
        loads[c].wait()
        window = jnp.concatenate(
            [
                x_buf[c, 8 + (k - 1) * local_rows : 8 + (k - 1) * local_rows + x_rows, :]
                for k in range(3)
            ],
            axis=1,
        )
        filtered = product(split(window), table, ((1,), (1,)))
        for device in range(devices):
            for tile in range(tiles):
                at = (device * tiles + tile) * local_rows
                send_one[device, tile, c * local_rows : (c + 1) * local_rows, :] = filtered[
                    at : at + local_rows, :
                ]

    pl.semaphore_wait(barrier, len(peers))
    step = tiles // CHUNKS
    copies = []
    for chunk in range(CHUNKS):
        part = pl.ds(chunk * step, step)
        for name, slot in zip(names, slots):
            copy = pltpu.make_async_remote_copy(
                src_ref=send_one.at[slot, part],
                dst_ref=recv_one.at[part, me],
                send_sem=send_one_sem.at[chunk, slot],
                recv_sem=recv_one_sem.at[chunk, me],
                device_id=name,
                device_id_type=pl.DeviceIdType.MESH,
            )
            copy.start()
            copies.append(copy)
    recv_one[:, me] = send_one[me]

    table = mixing_table(
        column_taps[...], channel_mix[...], chans, bands, local_channels, local_rows
    )
    mixing[0], mixing[1] = split(table)

    rows = step * local_rows
    for chunk in range(CHUNKS):
        part = pl.ds(chunk * step, step)
        for slot in slots:
            landed = recv_one.at[part, slot]
            pltpu.make_async_copy(landed, landed, recv_one_sem.at[chunk, slot]).wait()
        columns = jnp.concatenate(
            [
                recv_one[chunk * step + tile].reshape(mixing.shape[1], LANES)
                for tile in range(step)
            ],
            axis=1,
        )
        mixed = product((mixing[0], mixing[1]), split(columns), ((1,), (0,)))
        for device in range(devices):
            for c in range(local_channels):
                at = (device * local_channels + c) * local_rows
                for tile in range(step):
                    to = (chunk * step + tile) * local_rows
                    send_two[device, c, to : to + local_rows, :] = mixed[
                        at : at + local_rows, tile * LANES : (tile + 1) * LANES
                    ]
        here = pl.ds(chunk * rows, rows)
        there = pl.ds(pl.multiple_of(me * block_rows + chunk * rows, 8), rows)
        for name, slot in zip(names, slots):
            copy = pltpu.make_async_remote_copy(
                src_ref=send_two.at[slot, :, here],
                dst_ref=out_ref.at[:, there],
                send_sem=send_two_sem.at[chunk, slot],
                recv_sem=recv_two_sem.at[chunk, me],
                device_id=name,
                device_id_type=pl.DeviceIdType.MESH,
            )
            copy.start()
            copies.append(copy)
        out_ref[:, there, :] = send_two[me, :, chunk * rows : (chunk + 1) * rows, :]

    for chunk in range(CHUNKS):
        for slot in slots:
            landed = out_ref.at[
                :, pl.ds(pl.multiple_of(slot * block_rows + chunk * rows, 8), rows)
            ]
            pltpu.make_async_copy(landed, landed, recv_two_sem.at[chunk, slot]).wait()
    for copy in copies:
        copy.wait_send()


def fused(chans, bands, slide_region, row_taps, column_taps, channel_mix):
    local_channels, local_rows, width = slide_region.shape
    devices = chans * bands
    total_tiles = width // LANES
    tiles = total_tiles // devices
    block = local_channels * local_rows
    tiled = slide_region.reshape(local_channels, local_rows, total_tiles, LANES)
    tiled = tiled.transpose(0, 2, 1, 3).reshape(local_channels, total_tiles * local_rows, LANES)
    vmem = pl.BlockSpec(memory_space=pltpu.VMEM)
    anywhere = pl.BlockSpec(memory_space=pl.ANY)
    dma = pltpu.SemaphoreType.DMA
    out = pl.pallas_call(
        functools.partial(fused_kernel, chans, bands),
        out_shape=pltpu.VMEM(tiled.shape, jnp.float32),
        in_specs=[anywhere, vmem, vmem, vmem],
        out_specs=vmem,
        scratch_shapes=[
            pltpu.VMEM((local_channels, tiled.shape[1] + 16, LANES), jnp.float32),
            pltpu.VMEM((devices, tiles, block, LANES), jnp.float32),
            pltpu.VMEM((tiles, devices, block, LANES), jnp.float32),
            pltpu.VMEM((devices, local_channels, tiles * local_rows, LANES), jnp.float32),
            pltpu.VMEM((2, devices * block, devices * block), jnp.bfloat16),
            dma((local_channels,)),
            dma((CHUNKS, devices)),
            dma((CHUNKS, devices)),
            dma((CHUNKS, devices)),
            dma((CHUNKS, devices)),
        ],
        compiler_params=pltpu.CompilerParams(collective_id=0, has_side_effects=True),
    )(tiled, row_taps, column_taps, channel_mix)
    out = out.reshape(local_channels, total_tiles, local_rows, LANES)
    return out.transpose(0, 2, 1, 3).reshape(slide_region.shape)


def power_of_two(number):
    return number & (number - 1) == 0


def program(chans, bands, slide_region, row_taps, column_taps, channel_mix):
    local_channels, local_rows, width = slide_region.shape
    devices = chans * bands
    margin = (row_taps.shape[1] - 1) // 2
    fits = (
        power_of_two(chans)
        and power_of_two(bands)
        and width % (devices * LANES * CHUNKS) == 0
        and margin == LANES
        and column_taps.shape[1] == row_taps.shape[1]
        and local_rows == 4
        and local_rows * bands <= margin
        and local_channels * local_rows % 8 == 0
        and width // (devices * LANES * CHUNKS) * local_rows % 8 == 0
        and devices * local_channels * local_rows <= 512
    )
    if fits:
        return fused(chans, bands, slide_region, row_taps, column_taps, channel_mix)
    return on_device(slide_region, row_taps, column_taps, channel_mix)


def solution(mesh):
    in_specs = (P("chan", ("groups", "band"), None), P("chan", None), P(), P())
    out_specs = P("chan", ("groups", "band"), None)
    return jax.shard_map(
        functools.partial(program, mesh.shape["chan"], mesh.shape["band"]),
        mesh=mesh,
        in_specs=in_specs,
        out_specs=out_specs,
        check_vma=False,
    )
```

```python
import functools

import jax
import jax.numpy as jnp
from jax import lax
from jax.experimental import pallas as pl
from jax.experimental.pallas import tpu as pltpu
from jax.sharding import PartitionSpec as P

precise = lax.Precision.HIGHEST


def band_tables(filter_taps, tile_size):
    channels, length = filter_taps.shape
    margin = (length - 1) // 2
    period = 4 * tile_size
    border = 3 * tile_size + length
    widened = jnp.pad(filter_taps, ((0, 0), (border, border)))
    lowest = margin - tile_size + border
    window = widened[:, lowest : lowest + 3 * tile_size]
    vector = jnp.pad(window, ((0, 0), (0, tile_size)))
    repeated = jnp.tile(vector, (1, tile_size))[:, : tile_size * (period - 1)]
    toeplitz = repeated.reshape(channels, tile_size, period - 1)[:, :, : 3 * tile_size]
    stacked = jnp.transpose(toeplitz, (0, 2, 1))
    return stacked.reshape(channels, 3, tile_size, tile_size)


def along_columns(signal, filter_taps):
    tile_size = 128
    tables = band_tables(filter_taps, tile_size)
    channels, row_count, col_count = signal.shape
    tile_count = col_count // tile_size
    tiled = signal.reshape(channels, row_count, tile_count, tile_size)
    padded = jnp.pad(tiled, ((0, 0), (0, 0), (1, 1), (0, 0)))
    result = jnp.einsum(
        "crti,cij->crtj", padded[:, :, 0:tile_count], tables[:, 0], precision=precise
    )
    result = result + jnp.einsum(
        "crti,cij->crtj", padded[:, :, 1 : tile_count + 1], tables[:, 1], precision=precise
    )
    result = result + jnp.einsum(
        "crti,cij->crtj", padded[:, :, 2:], tables[:, 2], precision=precise
    )
    return result.reshape(channels, row_count, col_count)


def along_rows(signal, filter_taps):
    channels, row_count, col_count = signal.shape
    tile_size = 128 if row_count % 128 == 0 else row_count
    tables = band_tables(filter_taps, tile_size)
    tile_count = row_count // tile_size
    tiled = signal.reshape(channels, tile_count, tile_size, col_count)
    padded = jnp.pad(tiled, ((0, 0), (1, 1), (0, 0), (0, 0)))
    result = jnp.einsum("ctiw,cij->ctjw", padded[:, 0:tile_count], tables[:, 0], precision=precise)
    result = result + jnp.einsum(
        "ctiw,cij->ctjw", padded[:, 1 : tile_count + 1], tables[:, 1], precision=precise
    )
    result = result + jnp.einsum("ctiw,cij->ctjw", padded[:, 2:], tables[:, 2], precision=precise)
    return result.reshape(channels, row_count, col_count)


def on_device(slide_region, row_taps, column_taps, channel_mix):
    local_channels = slide_region.shape[0]
    across = along_columns(slide_region, row_taps)
    column_band = lax.all_to_all(across, "band", split_axis=2, concat_axis=1, tiled=True)
    first_channel = lax.axis_index("chan") * local_channels
    own_taps = lax.dynamic_slice_in_dim(column_taps, first_channel, local_channels, 0)
    vertical = along_rows(column_band, own_taps)
    own_mixing = lax.dynamic_slice_in_dim(channel_mix, first_channel, local_channels, 0)
    blended = jnp.einsum(
        "oc,chw->ohw",
        own_mixing,
        lax.all_gather(vertical, "chan", axis=0, tiled=True),
        precision=precise,
    )
    return lax.all_to_all(blended, "band", split_axis=1, concat_axis=2, tiled=True)


LANES = 128
CHUNKS = 2


def split(value):
    high = value.astype(jnp.bfloat16)
    return high, (value - high.astype(jnp.float32)).astype(jnp.bfloat16)


def product(left, right, dims):
    (left_high, left_low), (right_high, right_low) = left, right
    dot = functools.partial(
        lax.dot_general, dimension_numbers=(dims, ((), ())), preferred_element_type=jnp.float32
    )
    return dot(left_high, right_high) + (dot(left_low, right_high) + dot(left_high, right_low))


def filter_table(taps):
    shape = (LANES, LANES)
    lane = lax.broadcasted_iota(jnp.int32, shape, 1)
    row = lax.broadcasted_iota(jnp.int32, shape, 0)
    first, second = (
        pltpu.roll(
            jnp.broadcast_to(taps[:, at : at + LANES], shape), 0, 1, stride=1, stride_axis=0
        )
        for at in (0, LANES)
    )
    last = jnp.broadcast_to(taps[:, 2 * LANES :], shape)
    zero = jnp.zeros(shape, jnp.float32)
    return jnp.concatenate(
        [
            jnp.where(lane >= row, first, zero),
            jnp.where(lane >= row, second, first),
            jnp.where(lane == row, last, jnp.where(lane < row, second, zero)),
        ],
        axis=1,
    )


def mixing_table(column_taps, channel_mix, chans, bands, local_channels, local_rows):
    channels = chans * local_channels
    height = bands * local_rows
    block = local_channels * local_rows
    size = chans * bands * block
    margin = (column_taps.shape[1] - 1) // 2

    def coordinates(index):
        device, inner = index // block, index % block
        return (
            local_channels * (device % chans) + inner // local_rows,
            local_rows * (device // chans) + inner % local_rows,
        )

    tall = (size, channels)
    wide = (channels, size)
    pick_tall = (
        coordinates(lax.broadcasted_iota(jnp.int32, tall, 0))[0]
        == lax.broadcasted_iota(jnp.int32, tall, 1)
    ).astype(jnp.float32)
    pick_wide = (
        coordinates(lax.broadcasted_iota(jnp.int32, wide, 1))[0]
        == lax.broadcasted_iota(jnp.int32, wide, 0)
    ).astype(jnp.float32)
    weights = jnp.dot(
        jnp.dot(pick_tall, channel_mix, precision=precise), pick_wide, precision=precise
    )
    taps = lax.dot_general(
        column_taps[:, : 2 * margin],
        pick_wide,
        (((0,), (0,)), ((), ())),
        precision=precise,
    )
    square = (size, size)
    apart = (
        coordinates(lax.broadcasted_iota(jnp.int32, square, 1))[1]
        - coordinates(lax.broadcasted_iota(jnp.int32, square, 0))[1]
    )
    spread = jnp.zeros(square, jnp.float32)
    for distance in range(1 - height, height):
        at = margin + distance
        spread = jnp.where(apart == distance, taps[at : at + 1, :], spread)
    return weights * spread


def fused_kernel(
    chans, bands, x_hbm, row_taps, column_taps, channel_mix, out_ref,
    x_buf, tables, send_one, recv_one, send_two, mixing,
    ready, in_sem, send_one_sem, recv_one_sem, send_two_sem, recv_two_sem,
):
    local_channels, x_rows, _ = x_hbm.shape
    devices, _, block_rows, _ = send_two.shape
    tiles = send_one.shape[1]
    local_rows = block_rows // tiles
    chan, band = lax.axis_index("chan"), lax.axis_index("band")
    me = band * chans + chan

    half = bands // 2
    x_half = x_rows // 2
    peers = []
    for band_step in sorted(range(bands), key=lambda step: (step < half, step)):
        for chan_step in range(chans):
            if band_step or chan_step:
                to_chan, to_band = chan ^ chan_step, band ^ band_step
                slot = to_band * chans + to_chan
                name = {"chan": to_chan, "band": to_band}
                peers.append((name, slot))

    def each_peer(visit, also=None):
        for name, slot in peers:
            if also is None:
                visit(name, slot)
            else:
                pl.when(also(slot))(functools.partial(visit, name, slot))

    barrier = pltpu.get_barrier_semaphore()
    greet = functools.partial(
        pl.semaphore_signal, inc=1, device_id_type=pl.DeviceIdType.MESH
    )
    each_peer(lambda name, slot: greet(barrier, device_id=name), lambda slot: slot > me)
    loads = [
        pltpu.make_async_copy(x_hbm.at[c], x_buf.at[c, pl.ds(8, x_rows)], in_sem.at[c])
        for c in range(local_channels)
    ]
    for load in loads:
        load.start()

    @pl.when(me > 0)
    def _():
        pl.semaphore_wait(barrier, me)

    each_peer(lambda name, slot: greet(ready.at[me], device_id=name), lambda slot: slot < me)

    edge = jnp.zeros((8, LANES), jnp.float32)
    for c in range(local_channels):
        x_buf[c, 0:8, :] = edge
        x_buf[c, x_rows + 8 : x_rows + 16, :] = edge
        tables[c, 0], tables[c, 1] = split(filter_table(row_taps[c : c + 1, :]))

    def filter_half(which, first):
        start = pl.multiple_of(which * x_half, 8)
        for c in range(local_channels):
            if first:
                loads[c].wait()
            wide = x_buf[c, pl.ds(start, x_half + 16), :]
            window = jnp.concatenate(
                [
                    wide[8 + (k - 1) * local_rows : 8 + (k - 1) * local_rows + x_half]
                    for k in range(3)
                ],
                axis=1,
            )
            filtered = product(split(window), (tables[c, 0], tables[c, 1]), ((1,), (1,)))
            for device in range(devices // 2):
                for tile in range(tiles):
                    at = (device * tiles + tile) * local_rows
                    send_one[
                        which * (devices // 2) + device,
                        tile,
                        c * local_rows : (c + 1) * local_rows,
                        :,
                    ] = filtered[at : at + local_rows, :]

    step = tiles // CHUNKS

    def copy_one(chunk, name, slot):
        part = pl.ds(chunk * step, step)
        return pltpu.make_async_remote_copy(
            src_ref=send_one.at[slot, part],
            dst_ref=recv_one.at[part, me],
            send_sem=send_one_sem.at[chunk, slot],
            recv_sem=recv_one_sem.at[chunk, me],
            device_id=name,
            device_id_type=pl.DeviceIdType.MESH,
        )

    def send_one_to(chunk, name, slot):
        if chunk == 0:

            @pl.when(slot > me)
            def _():
                pl.semaphore_wait(ready.at[slot], 1)

        copy_one(chunk, name, slot).start()

    filter_half(1 - band // half, True)
    far = half * chans
    for name, slot in peers[:far]:
        send_one_to(0, name, slot)
    filter_half(band // half, False)
    for name, slot in peers[far:]:
        send_one_to(0, name, slot)
    for name, slot in peers:
        send_one_to(1, name, slot)
    recv_one[:, me] = send_one[me]

    table = mixing_table(
        column_taps[...], channel_mix[...], chans, bands, local_channels, local_rows
    )
    mixing[0], mixing[1] = split(table)

    rows = step * local_rows

    def copy_two(chunk, name, slot):
        return pltpu.make_async_remote_copy(
            src_ref=send_two.at[slot, :, pl.ds(chunk * rows, rows)],
            dst_ref=out_ref.at[
                :, pl.ds(pl.multiple_of(me * block_rows + chunk * rows, 8), rows)
            ],
            send_sem=send_two_sem.at[chunk, slot],
            recv_sem=recv_two_sem.at[chunk, me],
            device_id=name,
            device_id_type=pl.DeviceIdType.MESH,
        )

    for chunk in range(CHUNKS):
        part = pl.ds(chunk * step, step)
        def landed_one(name, slot):
            landed = recv_one.at[part, slot]
            pltpu.make_async_copy(landed, landed, recv_one_sem.at[chunk, slot]).wait()

        each_peer(landed_one)
        columns = jnp.concatenate(
            [
                recv_one[chunk * step + tile].reshape(mixing.shape[1], LANES)
                for tile in range(step)
            ],
            axis=1,
        )
        mixed = product((mixing[0], mixing[1]), split(columns), ((1,), (0,)))
        for device in range(devices):
            for c in range(local_channels):
                at = (device * local_channels + c) * local_rows
                for tile in range(step):
                    to = (chunk * step + tile) * local_rows
                    send_two[device, c, to : to + local_rows, :] = mixed[
                        at : at + local_rows, tile * LANES : (tile + 1) * LANES
                    ]
        there = pl.ds(pl.multiple_of(me * block_rows + chunk * rows, 8), rows)
        each_peer(lambda name, slot: copy_two(chunk, name, slot).start())
        out_ref[:, there, :] = send_two[me, :, chunk * rows : (chunk + 1) * rows, :]

    def finish(chunk, name, slot):
        landed = out_ref.at[
            :, pl.ds(pl.multiple_of(slot * block_rows + chunk * rows, 8), rows)
        ]
        pltpu.make_async_copy(landed, landed, recv_two_sem.at[chunk, slot]).wait()
        copy_one(chunk, name, slot).wait_send()
        copy_two(chunk, name, slot).wait_send()

    for chunk in range(CHUNKS):
        each_peer(functools.partial(finish, chunk))


def fused(chans, bands, slide_region, row_taps, column_taps, channel_mix):
    local_channels, local_rows, width = slide_region.shape
    devices = chans * bands
    total_tiles = width // LANES
    tiles = total_tiles // devices
    block = local_channels * local_rows
    tiled = slide_region.reshape(local_channels, local_rows, total_tiles, LANES)
    tiled = tiled.transpose(0, 2, 1, 3).reshape(local_channels, total_tiles * local_rows, LANES)
    vmem = pl.BlockSpec(memory_space=pltpu.VMEM)
    anywhere = pl.BlockSpec(memory_space=pl.ANY)
    dma = pltpu.SemaphoreType.DMA
    out = pl.pallas_call(
        functools.partial(fused_kernel, chans, bands),
        out_shape=pltpu.VMEM(tiled.shape, jnp.float32),
        in_specs=[anywhere, vmem, vmem, vmem],
        out_specs=vmem,
        scratch_shapes=[
            pltpu.VMEM((local_channels, tiled.shape[1] + 16, LANES), jnp.float32),
            pltpu.VMEM((local_channels, 2, LANES, 3 * LANES), jnp.bfloat16),
            pltpu.VMEM((devices, tiles, block, LANES), jnp.float32),
            pltpu.VMEM((tiles, devices, block, LANES), jnp.float32),
            pltpu.VMEM((devices, local_channels, tiles * local_rows, LANES), jnp.float32),
            pltpu.VMEM((2, devices * block, devices * block), jnp.bfloat16),
            pltpu.SemaphoreType.REGULAR((devices,)),
            dma((local_channels,)),
            dma((CHUNKS, devices)),
            dma((CHUNKS, devices)),
            dma((CHUNKS, devices)),
            dma((CHUNKS, devices)),
        ],
        compiler_params=pltpu.CompilerParams(collective_id=0, has_side_effects=True),
    )(tiled, row_taps, column_taps, channel_mix)
    out = out.reshape(local_channels, total_tiles, local_rows, LANES)
    return out.transpose(0, 2, 1, 3).reshape(slide_region.shape)


def power_of_two(number):
    return number & (number - 1) == 0


def program(chans, bands, slide_region, row_taps, column_taps, channel_mix):
    local_channels, local_rows, width = slide_region.shape
    devices = chans * bands
    margin = (row_taps.shape[1] - 1) // 2
    fits = (
        power_of_two(chans)
        and power_of_two(bands)
        and bands > 1
        and width % (devices * LANES * CHUNKS) == 0
        and margin == LANES
        and column_taps.shape[1] == row_taps.shape[1]
        and local_rows == 4
        and local_rows * bands <= margin
        and local_channels * local_rows % 8 == 0
        and width // (devices * LANES * CHUNKS) * local_rows % 8 == 0
        and devices * local_channels * local_rows <= 512
    )
    if fits:
        return fused(chans, bands, slide_region, row_taps, column_taps, channel_mix)
    return on_device(slide_region, row_taps, column_taps, channel_mix)


def solution(mesh):
    in_specs = (P("chan", ("groups", "band"), None), P("chan", None), P(), P())
    out_specs = P("chan", ("groups", "band"), None)
    return jax.shard_map(
        functools.partial(program, mesh.shape["chan"], mesh.shape["band"]),
        mesh=mesh,
        in_specs=in_specs,
        out_specs=out_specs,
        check_vma=False,
    )
```
